256 devices in a mesh: rows: 4 (over x), grid: 64 (over z, y, core).
Axes of the slice: x: 4, y: 4, z: 8, core: 2. Of those that a mesh axis runs over, the one named last changes fastest.
Arguments:
- positions: int32 [2, 2048], P(None, 'rows'), may hold values from 0 to 63, as said below
- angles: int32 [2, 32768], P(None, 'grid'), may hold values from 0 to 4095
- subspace: bfloat16 [2, 2048, 1920], P(None, 'rows', 'grid')
Outputs:
- spectrum: float32 [32768], P('grid')
The draws below stay inside these ranges and needn't reach their ends.
Inputs may be any that keep to these rules, and one draw needn't show every extreme that they name: `positions`: each column names a distinct lattice point; both coordinates lie in 0 to 63.
All inputs are finite; a program needn't handle non-finite values.
Results may differ from the reference program's by a relative error of at most 0.0012.
Values may be sent and summed in bfloat16 or wider, within the bound.
No kernel may reach another device: no remote copies, remote signals or barrier semaphores. Data moves between devices by JAX's collectives and lax.ppermute only.
A program may use at most 64 MiB of HBM per device.

```python
import math
import jax
import jax.numpy as jnp
from jax import lax

ELEMENTS = 2048
NOISE = 1920
SOURCES = 128
LATTICE = 64
PHASES = 4096
ANG_DEV = 512
ANGLES = 32768


def lattice_points(key):
    chosen = jax.random.permutation(jax.random.fold_in(key, 11), LATTICE * LATTICE)[:ELEMENTS]
    return jnp.stack([chosen // LATTICE, chosen % LATTICE]).astype(jnp.int32)


def grid_points(key):
    return jax.random.randint(jax.random.fold_in(key, 12), (2, ANGLES), 0, PHASES, dtype=jnp.int32)


def draw_positions(key, part):
    return lattice_points(key)


def draw_angles(key, part):
    return grid_points(key)


def draw_subspace(key, part):
    placed = lattice_points(key)
    grid_all = grid_points(key)
    chosen = jax.random.permutation(jax.random.fold_in(key, 13), ANGLES)[:SOURCES]
    source_angles = grid_all[:, chosen]
    phase_index = (placed[0][:, None] * source_angles[0][None, :] + placed[1][:, None] * source_angles[1][None, :]) % PHASES
    phase = phase_index.astype(jnp.float32) * (2.0 * math.pi / PHASES)
    source_re = jnp.cos(phase)
    source_im = jnp.sin(phase)
    spread = (2.0 * ELEMENTS) ** (-0.5)
    noise_re = spread * jax.random.normal(jax.random.fold_in(key, 14), (ELEMENTS, NOISE), jnp.float32)
    noise_im = spread * jax.random.normal(jax.random.fold_in(key, 15), (ELEMENTS, NOISE), jnp.float32)
    high = lax.Precision.HIGHEST
    coeff_re = (jnp.dot(source_re.T, noise_re, precision=high) + jnp.dot(source_im.T, noise_im, precision=high)) / ELEMENTS
    coeff_im = (jnp.dot(source_re.T, noise_im, precision=high) - jnp.dot(source_im.T, noise_re, precision=high)) / ELEMENTS
    result_re = noise_re - (jnp.dot(source_re, coeff_re, precision=high) - jnp.dot(source_im, coeff_im, precision=high))
    result_im = noise_im - (jnp.dot(source_re, coeff_im, precision=high) + jnp.dot(source_im, coeff_re, precision=high))
    return jnp.stack([result_re, result_im]).astype(jnp.bfloat16)


def setup_inputs(seed: int = 0) -> dict:
    splits = jax.random.split(jax.random.key(seed), 4)
    positions = draw_positions(jax.random.fold_in(splits[3], 71), 0)
    angles = draw_angles(jax.random.fold_in(splits[3], 71), 0)
    subspace = draw_subspace(jax.random.fold_in(splits[3], 71), 0)
    return dict(positions=positions, angles=angles, subspace=subspace)


def steering_block(positions, angle_block):
    phase_index = (positions[0][:, None] * angle_block[0][None, :] + positions[1][:, None] * angle_block[1][None, :]) % PHASES
    phase = phase_index.astype(jnp.float32) * (2.0 * math.pi / PHASES)
    return jnp.concatenate([jnp.cos(phase), jnp.sin(phase)], 0).astype(jnp.bfloat16)


def reference(positions, angles, subspace):
    real_part = subspace[0]
    imag_part = subspace[1]
    upper_half = jnp.concatenate([real_part, imag_part], 0)
    lower_half = jnp.concatenate([-imag_part, real_part], 0)
    stacked = jnp.stack([upper_half, lower_half]).astype(jnp.float32)
    blocks = ANGLES // ANG_DEV
    angle_blocks = jnp.transpose(angles.reshape(2, blocks, ANG_DEV), (1, 0, 2))

    def one_block(angle_block):
        steering = steering_block(positions, angle_block).astype(jnp.float32)
        projected = jnp.einsum("pmk,ma->pka", stacked, steering)
        squares = jnp.sum(projected * projected, axis=(0, 1))
        return 1.0 / (squares / NOISE + 1e-6)

    return lax.map(one_block, angle_blocks).reshape(ANGLES)
```

```python
import jax
import jax.numpy as jnp
from jax import lax
from jax.sharding import Mesh
from jax.sharding import PartitionSpec as P

NOISE = 1920
PHASES = 4096
ROWS, FAR, NEAR, SIDE, CORE = "rows", "far", "near", "side", "core"
GRID = (FAR, NEAR, SIDE, CORE)


def sine_coefficients():
    import numpy as np

    nodes = 0.03125 * (1.0 - np.cos((np.arange(64) + 0.5) * np.pi / 64))
    root = np.sqrt(nodes)
    value = np.sin(2.0 * np.pi * root) / root
    return tuple(float(c) for c in np.polynomial.polynomial.polyfit(nodes, value, 5))


SINE = sine_coefficients()


def sine_of(u):
    square = u * u
    total = jnp.full_like(u, SINE[-1])
    for c in SINE[-2::-1]:
        total = total * square + c
    return total * u


def cos_sin_of(turns):
    rest = turns - jnp.round(turns)
    cos = sine_of(0.25 - jnp.abs(rest))
    sin = sine_of(jnp.maximum(jnp.minimum(rest, 0.5 - rest), -0.5 - rest))
    return cos, sin


def body(positions, angles, subspace):
    rows, far = lax.axis_size(ROWS), lax.axis_size(FAR)
    near, side = lax.axis_size(NEAR), lax.axis_size(SIDE)
    mine = jnp.concatenate([positions, angles], 0)
    lists = lax.all_to_all(
        jnp.broadcast_to(mine[None], (rows * far, *mine.shape)), (ROWS, FAR), 0, 0, tiled=True
    ).reshape(rows, far, *mine.shape)
    coords = jnp.moveaxis(lists[:, 0, :2], 1, 0).reshape(2, -1).astype(jnp.float32)
    turns = jnp.moveaxis(lists[0, :, 2:], 1, 0).reshape(2, -1).astype(jnp.float32) * (1.0 / PHASES)

    width = subspace.shape[2]
    quarter = -(-width // rows)
    columns = jnp.pad(subspace, ((0, 0), (0, 0), (0, rows * quarter - width)))
    columns = columns.reshape(2, -1, rows, quarter).transpose(2, 0, 3, 1)
    columns = columns.reshape(rows, 1, 2 * quarter, -1)
    pieces = jnp.broadcast_to(columns, (rows, near * side, *columns.shape[2:]))
    pieces = pieces.reshape(rows * near * side, *columns.shape[2:])
    got = lax.all_to_all(pieces, (ROWS, NEAR, SIDE), 0, 0, tiled=True)
    other = lax.ppermute(got, CORE, [(0, 1), (1, 0)])
    both = jnp.stack([got, other])
    both = both.reshape(2, rows, near * side, 2, quarter, -1)

    cos, sin = cos_sin_of(coords[0][:, None] * turns[0][None] + coords[1][:, None] * turns[1][None])
    steering = jnp.concatenate([cos.astype(jnp.bfloat16), sin.astype(jnp.bfloat16)], 1)
    weights = both.transpose(3, 0, 2, 4, 1, 5).reshape(-1, cos.shape[0])
    projected = jnp.dot(weights, steering, preferred_element_type=jnp.float32)
    projected = projected.reshape(2, -1, 2, cos.shape[1])
    real = projected[0, :, 0] + projected[1, :, 1]
    imag = projected[0, :, 1] - projected[1, :, 0]
    sums = jnp.sum(real * real + imag * imag, 0)

    sums = jnp.broadcast_to(sums.reshape(1, far, -1), (rows, far, sums.size // far))
    parts = lax.all_to_all(sums.reshape(rows * far, -1), (ROWS, FAR), 0, 0, tiled=True)
    return 1.0 / (jnp.sum(parts, 0) / NOISE + 1e-06)


def solution(mesh):
    split = Mesh(mesh.devices.reshape(mesh.shape["rows"], 4, 2, 4, 2), (ROWS, *GRID))
    in_specs = (P(None, ROWS), P(None, GRID), P(None, ROWS, GRID))
    return jax.shard_map(body, mesh=split, in_specs=in_specs, out_specs=P(GRID), check_vma=False)
```

```python
import jax
import jax.numpy as jnp
import numpy as np
from jax import lax
from jax.experimental import pallas as pl
from jax.experimental.pallas import tpu as pltpu
from jax.sharding import Mesh
from jax.sharding import PartitionSpec as P

NOISE = 1920
PHASES = 4096
LATTICE = 64
LANES = 128
BATCH = 32
PITCH = 36
ROWS, FAR, NEAR, SIDE, CORE = "rows", "far", "near", "side", "core"
GRID = (FAR, NEAR, SIDE, CORE)


def sine_coefficients():
    nodes = 0.03125 * (1.0 - np.cos((np.arange(64) + 0.5) * np.pi / 64))
    root = np.sqrt(nodes)
    value = np.sin(2.0 * np.pi * root) / root
    return tuple(float(c) for c in np.polynomial.polynomial.polyfit(nodes, value, 5))


SINE = sine_coefficients()


def sine_of(u):
    square = u * u
    total = jnp.full_like(u, SINE[-1])
    for c in SINE[-2::-1]:
        total = total * square + c
    return total * u


def cos_sin_of(turns):
    rest = turns - jnp.round(turns)
    cos = sine_of(0.25 - jnp.abs(rest))
    sin = sine_of(jnp.maximum(jnp.minimum(rest, 0.5 - rest), -0.5 - rest))
    return cos, sin


def steering_kernel(rows_ref, turns_ref, out_ref, table, stage):
    blocks = turns_ref.shape[1]

    def fill(step, carry):
        for k in range(2):
            cos, sin = cos_sin_of(turns_ref[k] * step.astype(jnp.float32))
            here = pl.ds(pl.multiple_of(step * blocks, blocks), blocks)
            table[2 * k, here, :] = cos
            table[2 * k + 1, here, :] = sin
        return carry

    lax.fori_loop(0, LATTICE, fill, 0, unroll=4)

    def batch(step, carry):
        first = pl.multiple_of(step * BATCH, BATCH)
        for e in range(BATCH):
            one = pl.ds(pl.multiple_of(rows_ref[0, first + e], blocks), blocks)
            two = pl.ds(pl.multiple_of(rows_ref[1, first + e], blocks), blocks)
            cos_one, sin_one = table[0, one, :], table[1, one, :]
            cos_two, sin_two = table[2, two, :], table[3, two, :]
            stage[0, pl.ds(e, blocks, stride=PITCH), :] = cos_one * cos_two - sin_one * sin_two
            stage[1, pl.ds(e, blocks, stride=PITCH), :] = sin_one * cos_two + cos_one * sin_two
        for k in range(2):
            for b in range(blocks):
                part = stage[k, b * PITCH : b * PITCH + BATCH, :]
                out_ref[k, b, pl.ds(first, BATCH), :] = part.astype(out_ref.dtype)
        return carry

    lax.fori_loop(0, out_ref.shape[2] // BATCH, batch, 0)


def steering_of(table_rows, turns):
    blocks, elements = turns.shape[1], table_rows.shape[1]
    return pl.pallas_call(
        steering_kernel,
        out_shape=pltpu.VMEM((2, blocks, elements, LANES), jnp.bfloat16),
        in_specs=[
            pl.BlockSpec(memory_space=pltpu.SMEM),
            pl.BlockSpec(memory_space=pltpu.VMEM),
        ],
        out_specs=pl.BlockSpec(memory_space=pltpu.VMEM),
        scratch_shapes=[
            pltpu.VMEM((4, LATTICE * blocks, LANES), jnp.float32),
            pltpu.VMEM((2, blocks * PITCH, LANES), jnp.float32),
        ],
        cost_estimate=pl.CostEstimate(
            flops=6 * blocks * elements * LANES, bytes_accessed=0, transcendentals=0
        ),
        compiler_params=pltpu.CompilerParams(vmem_limit_bytes=24 * 2**20),
        name="steering",
    )(table_rows, turns)


def sums_kernel(own_ref, other_ref, steering_ref, out_ref):
    weights = [
        jnp.concatenate([ref[r] for r in range(ref.shape[0])], 1) for ref in (own_ref, other_ref)
    ]
    weights = jnp.concatenate(weights, 0)
    for b in range(steering_ref.shape[1]):
        both = jnp.concatenate([steering_ref[0, b], steering_ref[1, b]], 1)
        product = jnp.dot(weights, both, preferred_element_type=jnp.float32)
        total = jnp.zeros((8, LANES), jnp.float32)
        for g in range(0, product.shape[0], 16):
            upper, lower = product[g : g + 8], product[g + 8 : g + 16]
            real = upper[:, :LANES] + lower[:, LANES:]
            imag = upper[:, LANES:] - lower[:, :LANES]
            total = total + (real * real + imag * imag)
        out_ref[b : b + 1, :] = jnp.sum(total, 0, keepdims=True)


def sums_of(own, other, steering):
    blocks = steering.shape[1]
    return pl.pallas_call(
        sums_kernel,
        out_shape=jax.ShapeDtypeStruct((blocks, LANES), jnp.float32),
        in_specs=[pl.BlockSpec(memory_space=pltpu.VMEM)] * 3,
        out_specs=pl.BlockSpec(memory_space=pltpu.VMEM),
        cost_estimate=pl.CostEstimate(
            flops=8 * own.shape[1] * own.shape[0] * own.shape[2] * blocks * LANES,
            bytes_accessed=0,
            transcendentals=0,
        ),
        compiler_params=pltpu.CompilerParams(vmem_limit_bytes=24 * 2**20),
        name="sums",
    )(own, other, steering)


def body(positions, angles, subspace):
    rows, far = lax.axis_size(ROWS), lax.axis_size(FAR)
    near, side = lax.axis_size(NEAR), lax.axis_size(SIDE)
    mine = jnp.concatenate([positions, angles], 0)
    lists = lax.all_to_all(
        jnp.broadcast_to(mine[None], (rows * far, *mine.shape)), (ROWS, FAR), 0, 0, tiled=True
    ).reshape(rows, far, *mine.shape)
    blocks = far * angles.shape[1] // LANES
    table_rows = jnp.moveaxis(lists[:, 0, :2], 1, 0).reshape(2, -1) * blocks
    turns = jnp.moveaxis(lists[0, :, 2:], 1, 0).reshape(2, blocks, LANES)
    steering = steering_of(table_rows, turns.astype(jnp.float32) * (1.0 / PHASES))

    width = subspace.shape[2]
    quarter = -(-width // rows)
    columns = jnp.pad(subspace, ((0, 0), (0, 0), (0, rows * quarter - width)))
    columns = columns.reshape(2, -1, rows, quarter).transpose(2, 0, 3, 1)
    columns = columns.reshape(rows, 1, 2 * quarter, -1)
    pieces = jnp.broadcast_to(columns, (rows, near * side, *columns.shape[2:]))
    pieces = pieces.reshape(rows * near * side, *columns.shape[2:])
    own = lax.all_to_all(pieces, (ROWS, NEAR, SIDE), 0, 0, tiled=True)
    other = lax.ppermute(own, CORE, [(0, 1), (1, 0)])
    own, other = (part.reshape(rows, -1, part.shape[2]) for part in (own, other))

    sums = sums_of(own, other, steering).reshape(1, far, -1)
    sums = jnp.broadcast_to(sums, (rows, *sums.shape[1:]))
    parts = lax.all_to_all(sums.reshape(rows * far, -1), (ROWS, FAR), 0, 0, tiled=True)
    return 1.0 / (jnp.sum(parts, 0) / NOISE + 1e-06)


def solution(mesh):
    split = Mesh(mesh.devices.reshape(mesh.shape["rows"], 4, 2, 4, 2), (ROWS, *GRID))
    in_specs = (P(None, ROWS), P(None, GRID), P(None, ROWS, GRID))
    return jax.shard_map(body, mesh=split, in_specs=in_specs, out_specs=P(GRID), check_vma=False)
```

```python
import jax
import jax.numpy as jnp
import numpy as np
from jax import lax
from jax.experimental import pallas as pl
from jax.experimental.pallas import tpu as pltpu
from jax.sharding import Mesh
from jax.sharding import PartitionSpec as P

NOISE = 1920
PHASES = 4096
LATTICE = 64
DIGIT = 6
LANES = 128
BATCH = 32
EXTRA = 4
ROWS, DEEP, SIDE, CORE = "rows", "deep", "side", "core"
GRID = (DEEP, SIDE, CORE)


def sine_coefficients():
    nodes = 0.03125 * (1.0 - np.cos((np.arange(64) + 0.5) * np.pi / 64))
    root = np.sqrt(nodes)
    value = np.sin(2.0 * np.pi * root) / root
    return tuple(float(c) for c in np.polynomial.polynomial.polyfit(nodes, value, 5))


SINE = sine_coefficients()


def sine_of(u):
    square = u * u
    total = jnp.full_like(u, SINE[-1])
    for c in SINE[-2::-1]:
        total = total * square + c
    return total * u


def cos_sin_of(turns):
    rest = turns - jnp.round(turns)
    cos = sine_of(0.25 - jnp.abs(rest))
    sin = sine_of(jnp.maximum(jnp.minimum(rest, 0.5 - rest), -0.5 - rest))
    return cos, sin


def pack_kernel(positions_ref, angles_ref, columns_ref, out_ref):
    group, pairs, _, share = out_ref.shape
    each, width = pairs - 3, columns_ref.shape[0]
    angles = angles_ref[...]
    lists = (positions_ref[...], angles >> DIGIT, angles & (LATTICE - 1))
    lists = [part.astype(jnp.float32).astype(out_ref.dtype) for part in lists]
    for g in range(group):
        for c in range(each):
            if g * each + c < width:
                out_ref[g, c] = columns_ref[g * each + c]
            else:
                out_ref[g, c] = jnp.zeros((2, share), out_ref.dtype)
        for k in range(3):
            out_ref[g, each + k] = lists[k]


def packed(positions, angles, columns, group):
    width, _, share = columns.shape
    pairs = -(-width // group) + 3
    return pl.pallas_call(
        pack_kernel,
        out_shape=jax.ShapeDtypeStruct((group, pairs, 2, share), columns.dtype),
        in_specs=[pl.BlockSpec(memory_space=pltpu.VMEM)] * 3,
        out_specs=pl.BlockSpec(memory_space=pltpu.VMEM),
        cost_estimate=pl.CostEstimate(flops=2**16, bytes_accessed=0, transcendentals=0),
        name="pack",
    )(positions, angles, columns)


def rows_kernel(lists_ref, rows_ref):
    row_groups, side, pairs, _, share = lists_ref.shape
    scale = 2 * side * share // LANES
    for r in range(row_groups):
        coordinates = lists_ref[r, 0, pairs - 3].astype(jnp.float32) * scale
        rows_ref[:, r * share : (r + 1) * share] = coordinates.astype(jnp.int32)


def tables_kernel(lists_ref, table_ref, turns):
    _, side, pairs, _, share = lists_ref.shape
    blocks = turns.shape[1]
    for s in range(side):
        high = lists_ref[0, s, pairs - 2].astype(jnp.float32)
        low = lists_ref[0, s, pairs - 1].astype(jnp.float32)
        part = high * (LATTICE / PHASES) + low * (1.0 / PHASES)
        for j in range(share // LANES):
            b = s * (share // LANES) + j
            for k in range(2):
                turns[k, b : b + 1, :] = part[k : k + 1, j * LANES : (j + 1) * LANES]

    def fill(step, carry):
        for k in range(2):
            cos, sin = cos_sin_of(turns[k] * step.astype(jnp.float32))
            first = pl.multiple_of(2 * step * blocks, 2 * blocks)
            table_ref[k, pl.ds(first, blocks), :] = cos
            table_ref[k, pl.ds(first + blocks, blocks), :] = sin
        return carry

    lax.fori_loop(0, LATTICE, fill, 0, unroll=4)


def tables_of(lists):
    row_groups, side, _, _, share = lists.shape
    blocks = side * share // LANES
    rows = pl.pallas_call(
        rows_kernel,
        out_shape=pltpu.VMEM((2, row_groups * share), jnp.int32),
        in_specs=[pl.BlockSpec(memory_space=pltpu.VMEM)],
        out_specs=pl.BlockSpec(memory_space=pltpu.VMEM),
        name="rows",
    )(lists)
    table = pl.pallas_call(
        tables_kernel,
        out_shape=pltpu.VMEM((2, LATTICE * 2 * blocks, LANES), jnp.float32),
        in_specs=[pl.BlockSpec(memory_space=pltpu.VMEM)],
        out_specs=pl.BlockSpec(memory_space=pltpu.VMEM),
        scratch_shapes=[pltpu.VMEM((2, blocks, LANES), jnp.float32)],
        cost_estimate=pl.CostEstimate(flops=2**22, bytes_accessed=0, transcendentals=0),
        compiler_params=pltpu.CompilerParams(vmem_limit_bytes=4 * 2**20),
        name="tables",
    )(lists)
    return table, rows


def sums_kernel(rows_ref, table_ref, own_ref, other_ref, out_ref, steering):
    deep, row_groups, _, _, share = own_ref.shape
    blocks, elements = out_ref.shape[0], row_groups * share
    pitch = elements + EXTRA

    def batch(step, carry):
        first = pl.multiple_of(step * BATCH, BATCH)
        for e in range(BATCH):
            one = pl.multiple_of(rows_ref[0, first + e], 2 * blocks)
            two = pl.multiple_of(rows_ref[1, first + e], 2 * blocks)
            cos_one, sin_one = jnp.split(table_ref[0, pl.ds(one, 2 * blocks), :], 2)
            cos_two, sin_two = jnp.split(table_ref[1, pl.ds(two, 2 * blocks), :], 2)
            here = pl.ds(first + e, blocks, stride=pitch)
            steering[0, here, :] = cos_one * cos_two - sin_one * sin_two
            steering[1, here, :] = sin_one * cos_two + cos_one * sin_two
        return carry

    lax.fori_loop(0, elements // BATCH, batch, 0)

    weights = jnp.concatenate(
        [
            jnp.concatenate([ref[d, r].reshape(-1, share) for r in range(row_groups)], 1)
            for ref in (own_ref, other_ref)
            for d in range(deep)
        ],
        0,
    )
    is_real = lax.broadcasted_iota(jnp.int32, (8, LANES), 0) % 2 == 0
    for b in range(blocks):
        both = [
            steering[k, b * pitch : b * pitch + elements, :].astype(weights.dtype) for k in range(2)
        ]
        both = jnp.concatenate(both, 1)
        product = jnp.dot(weights, both, preferred_element_type=jnp.float32)
        total = jnp.zeros((8, LANES), jnp.float32)
        for g in range(0, product.shape[0], 8):
            cos, sin = product[g : g + 8, :LANES], product[g : g + 8, LANES:]
            real = cos + pltpu.roll(sin, 7, 0)
            imag = sin - pltpu.roll(cos, 7, 0)
            total = total + (real * real + imag * imag)
        out_ref[b : b + 1, :] = jnp.sum(jnp.where(is_real, total, 0.0), 0, keepdims=True)


def sums_of(table, rows, own, other):
    blocks = table.shape[1] // (2 * LATTICE)
    return pl.pallas_call(
        sums_kernel,
        out_shape=jax.ShapeDtypeStruct((blocks, LANES), jnp.float32),
        in_specs=[pl.BlockSpec(memory_space=pltpu.SMEM)]
        + [pl.BlockSpec(memory_space=pltpu.VMEM)] * 3,
        out_specs=pl.BlockSpec(memory_space=pltpu.VMEM),
        scratch_shapes=[pltpu.VMEM((2, blocks * (rows.shape[1] + EXTRA), LANES), jnp.float32)],
        cost_estimate=pl.CostEstimate(
            flops=8 * own.size * blocks * LANES, bytes_accessed=0, transcendentals=0
        ),
        compiler_params=pltpu.CompilerParams(vmem_limit_bytes=44 * 2**20),
        name="sums",
    )(rows, table, own, other)


def body(positions, angles, subspace):
    rows, side, deep = lax.axis_size(ROWS), lax.axis_size(SIDE), lax.axis_size(DEEP)
    group = rows * side
    share, width = subspace.shape[1:]
    each = -(-width // group)
    pieces = packed(positions, angles, subspace.transpose(2, 0, 1), group)
    got = lax.all_to_all(pieces, (ROWS, SIDE), 0, 0, tiled=True)
    got = got.reshape(rows, side, *pieces.shape[1:])

    columns = got[:, :, :each].reshape(1, rows, side * each, 2, share)
    columns = jnp.broadcast_to(columns, (deep, *columns.shape[1:]))
    own = lax.all_to_all(columns, DEEP, 0, 0, tiled=True)
    other = lax.ppermute(own, CORE, [(0, 1), (1, 0)])

    table, table_rows = tables_of(got)
    sums = sums_of(table, table_rows, own, other).reshape(1, side, -1)
    sums = jnp.broadcast_to(sums, (rows, *sums.shape[1:]))
    parts = lax.all_to_all(sums.reshape(group, -1), (ROWS, SIDE), 0, 0, tiled=True)
    return 1.0 / (jnp.sum(parts, 0) / NOISE + 1e-06)


def solution(mesh):
    split = Mesh(mesh.devices.reshape(mesh.shape["rows"], 8, 4, 2), (ROWS, *GRID))
    in_specs = (P(None, ROWS), P(None, GRID), P(None, ROWS, GRID))
    return jax.shard_map(body, mesh=split, in_specs=in_specs, out_specs=P(GRID), check_vma=False)
```

```python
import functools

import jax
import jax.numpy as jnp
import numpy as np
from jax import lax
from jax.experimental import pallas as pl
from jax.experimental.pallas import tpu as pltpu
from jax.sharding import Mesh
from jax.sharding import PartitionSpec as P

NOISE = 1920
PHASES = 4096
LATTICE = 64
LANES = 128
BATCH = 32
EXTRA = 4
ROWS, DEEP, SIDE, CORE = "rows", "deep", "side", "core"
GRID = (DEEP, SIDE, CORE)


def sine_coefficients():
    nodes = 0.03125 * (1.0 - np.cos((np.arange(64) + 0.5) * np.pi / 64))
    root = np.sqrt(nodes)
    value = np.sin(2.0 * np.pi * root) / root
    return tuple(float(c) for c in np.polynomial.polynomial.polyfit(nodes, value, 5))


SINE = sine_coefficients()


def sine_of(u):
    square = u * u
    total = jnp.full_like(u, SINE[-1])
    for c in SINE[-2::-1]:
        total = total * square + c
    return total * u


def cos_sin_of(turns):
    rest = turns - jnp.round(turns)
    cos = sine_of(0.25 - jnp.abs(rest))
    sin = sine_of(jnp.maximum(jnp.minimum(rest, 0.5 - rest), -0.5 - rest))
    return cos, sin


def pack_kernel(positions_ref, columns_ref, out_ref):
    row_groups, deep, tiles = out_ref.shape[0], out_ref.shape[1], positions_ref.shape[0]
    quarter, width = (out_ref.shape[2] - 1) // tiles, columns_ref.shape[0]
    mine = positions_ref[lax.rem(lax.axis_index(DEEP), tiles)]
    mine = mine.astype(jnp.float32).astype(out_ref.dtype)
    nothing = jnp.zeros((2, LANES), out_ref.dtype)
    for r in range(row_groups):
        for c in range(quarter):
            column = r * quarter + c
            for t in range(tiles):
                part = columns_ref[column, :, t * LANES : (t + 1) * LANES] if column < width else nothing
                for d in range(deep):
                    out_ref[r, d, t * quarter + c] = part
        for d in range(deep):
            out_ref[r, d, tiles * quarter] = mine


def packed(positions, columns, row_groups, deep):
    width, tiles = columns.shape[0], positions.shape[0]
    pairs = tiles * -(-width // row_groups) + 1
    return pl.pallas_call(
        pack_kernel,
        out_shape=jax.ShapeDtypeStruct((row_groups, deep, pairs, 2, LANES), columns.dtype),
        in_specs=[pl.BlockSpec(memory_space=pltpu.VMEM)] * 2,
        out_specs=pl.BlockSpec(memory_space=pltpu.VMEM),
        cost_estimate=pl.CostEstimate(flops=2**16, bytes_accessed=0, transcendentals=0),
        name="pack",
    )(positions, columns)


def rows_kernel(own_ref, rows_ref, *, scale):
    row_groups, _, pairs, _, _ = own_ref.shape
    elements = rows_ref.shape[0] // 2
    tiles = elements // (row_groups * LANES)
    for r in range(row_groups):
        for t in range(tiles):
            part = (own_ref[r, t, pairs - 1].astype(jnp.float32) * scale).astype(jnp.int32)
            for k in range(2):
                here = k * elements + (r * tiles + t) * LANES
                rows_ref[here : here + LANES] = part[k]


def turns_kernel(*refs):
    *angles, turns_ref = refs
    side, share = len(angles), angles[0].shape[1]
    each = share // LANES
    for s, ref in enumerate(angles):
        first = lax.rem(lax.axis_index(SIDE) + side - s, side) * each
        part = ref[...].astype(jnp.float32) * (1.0 / PHASES)
        for j in range(each):
            for k in range(2):
                turns_ref[k, pl.ds(first + j, 1), :] = part[k : k + 1, j * LANES : (j + 1) * LANES]


def tables_kernel(turns_ref, table_ref):
    blocks = turns_ref.shape[1]

    def fill(step, carry):
        for k in range(2):
            cos, sin = cos_sin_of(turns_ref[k] * step.astype(jnp.float32))
            first = pl.multiple_of(2 * step * blocks, 2 * blocks)
            table_ref[k, pl.ds(first, blocks), :] = cos
            table_ref[k, pl.ds(first + blocks, blocks), :] = sin
        return carry

    lax.fori_loop(0, LATTICE, fill, 0, unroll=4)


def rows_of(own, elements, blocks):
    return pl.pallas_call(
        functools.partial(rows_kernel, scale=2 * blocks),
        out_shape=pltpu.VMEM((2 * elements,), jnp.int32),
        in_specs=[pl.BlockSpec(memory_space=pltpu.VMEM)],
        out_specs=pl.BlockSpec(memory_space=pltpu.VMEM),
        name="rows",
    )(own)


def turns_of(angles):
    blocks = len(angles) * angles[0].shape[1] // LANES
    return pl.pallas_call(
        turns_kernel,
        out_shape=jax.ShapeDtypeStruct((2, blocks, LANES), jnp.float32),
        in_specs=[pl.BlockSpec(memory_space=pltpu.VMEM)] * len(angles),
        out_specs=pl.BlockSpec(memory_space=pltpu.VMEM),
        cost_estimate=pl.CostEstimate(flops=2**16, bytes_accessed=0, transcendentals=0),
        name="turns",
    )(*angles)


def tables_of(turns):
    return pl.pallas_call(
        tables_kernel,
        out_shape=pltpu.VMEM((2, LATTICE * 2 * turns.shape[1], LANES), jnp.float32),
        in_specs=[pl.BlockSpec(memory_space=pltpu.VMEM)],
        out_specs=pl.BlockSpec(memory_space=pltpu.VMEM),
        cost_estimate=pl.CostEstimate(flops=2**22, bytes_accessed=0, transcendentals=0),
        compiler_params=pltpu.CompilerParams(vmem_limit_bytes=4 * 2**20),
        name="tables",
    )(turns)


def sums_kernel(rows_ref, table_ref, own_ref, other_ref, out_ref, steering):
    row_groups, deep, pairs, _, _ = own_ref.shape
    blocks, elements = out_ref.shape[0], rows_ref.shape[0] // 2
    tiles = elements // (row_groups * LANES)
    quarter = (pairs - 1) // tiles
    pitch = elements + EXTRA

    def batch(step, carry):
        first = pl.multiple_of(step * BATCH, BATCH)
        for e in range(BATCH):
            one = pl.multiple_of(rows_ref[first + e], 2 * blocks)
            two = pl.multiple_of(rows_ref[elements + first + e], 2 * blocks)
            cos_one, sin_one = jnp.split(table_ref[0, pl.ds(one, 2 * blocks), :], 2)
            cos_two, sin_two = jnp.split(table_ref[1, pl.ds(two, 2 * blocks), :], 2)
            here = pl.ds(first + e, blocks, stride=pitch)
            steering[0, here, :] = cos_one * cos_two - sin_one * sin_two
            steering[1, here, :] = sin_one * cos_two + cos_one * sin_two
        return carry

    lax.fori_loop(0, elements // BATCH, batch, 0)

    weights = [
        [
            ref[r, d, t * quarter : (t + 1) * quarter].reshape(2 * quarter, LANES)
            for r in range(row_groups)
            for t in range(tiles)
        ]
        for ref in (own_ref, other_ref)
        for d in range(deep)
    ]
    weights = jnp.concatenate([jnp.concatenate(part, 1) for part in weights], 0)
    is_real = lax.broadcasted_iota(jnp.int32, (8, LANES), 0) % 2 == 0
    for b in range(blocks):
        both = [
            steering[k, b * pitch : b * pitch + elements, :].astype(weights.dtype) for k in range(2)
        ]
        both = jnp.concatenate(both, 1)
        product = jnp.dot(weights, both, preferred_element_type=jnp.float32)
        total = jnp.zeros((8, LANES), jnp.float32)
        for g in range(0, product.shape[0], 8):
            cos, sin = product[g : g + 8, :LANES], product[g : g + 8, LANES:]
            real = cos + pltpu.roll(sin, 7, 0)
            imag = sin - pltpu.roll(cos, 7, 0)
            total = total + (real * real + imag * imag)
        out_ref[b : b + 1, :] = jnp.sum(jnp.where(is_real, total, 0.0), 0, keepdims=True)


def sums_of(table, rows, own, other):
    blocks = table.shape[1] // (2 * LATTICE)
    return pl.pallas_call(
        sums_kernel,
        out_shape=jax.ShapeDtypeStruct((blocks, LANES), jnp.float32),
        in_specs=[pl.BlockSpec(memory_space=pltpu.SMEM)]
        + [pl.BlockSpec(memory_space=pltpu.VMEM)] * 3,
        out_specs=pl.BlockSpec(memory_space=pltpu.VMEM),
        scratch_shapes=[pltpu.VMEM((2, blocks * (rows.size // 2 + EXTRA), LANES), jnp.float32)],
        cost_estimate=pl.CostEstimate(
            flops=8 * own.size * blocks * LANES, bytes_accessed=0, transcendentals=0
        ),
        compiler_params=pltpu.CompilerParams(vmem_limit_bytes=36 * 2**20),
        name="sums",
    )(rows, table, own, other)


def spectrum_of(positions, angles, subspace):
    rows, side, deep = lax.axis_size(ROWS), lax.axis_size(SIDE), lax.axis_size(DEEP)
    tiles = positions.shape[1] // LANES
    coordinates = positions.reshape(2, tiles, LANES).transpose(1, 0, 2)
    pieces = packed(coordinates, subspace.transpose(2, 0, 1), rows, deep)
    own = lax.all_to_all(
        pieces.reshape(rows * deep, *pieces.shape[2:]), (ROWS, DEEP), 0, 0, tiled=True
    )
    turned = [angles]
    for step in range(1, side):
        moves = [(s, (s + step) % side) for s in range(side)]
        turned.append(lax.ppermute(angles, SIDE, moves))
    other = lax.ppermute(own, CORE, [(0, 1), (1, 0)])
    own, other = (part.reshape(pieces.shape) for part in (own, other))

    table = tables_of(turns_of(turned))
    table_rows = rows_of(own, rows * positions.shape[1], table.shape[1] // (2 * LATTICE))
    sums = sums_of(table, table_rows, own, other).reshape(1, side, -1)
    sums = jnp.broadcast_to(sums, (rows, *sums.shape[1:]))
    parts = lax.all_to_all(sums.reshape(rows * side, -1), (ROWS, SIDE), 0, 0, tiled=True)
    return 1.0 / (jnp.sum(parts, 0) / NOISE + 1e-06)


def solution(mesh):
    split = Mesh(mesh.devices.reshape(mesh.shape["rows"], 8, 4, 2), (ROWS, *GRID))
    in_specs = (P(None, ROWS), P(None, GRID), P(None, ROWS, GRID))
    return jax.shard_map(spectrum_of, mesh=split, in_specs=in_specs, out_specs=P(GRID), check_vma=False)
```

```python
import jax
import jax.numpy as jnp
import numpy as np
from jax import lax
from jax.experimental import pallas as pl
from jax.experimental.pallas import tpu as pltpu
from jax.sharding import Mesh
from jax.sharding import PartitionSpec as P

NOISE = 1920
PHASES = 4096
LATTICE = 64
LANES = 128
BATCH = 32
PITCH = BATCH + 4
ROWS, FAR, NEAR, SIDE, CORE = "rows", "far", "near", "side", "core"
GRID = (FAR, NEAR, SIDE, CORE)


def sine_coefficients():
    nodes = 0.03125 * (1.0 - np.cos((np.arange(64) + 0.5) * np.pi / 64))
    root = np.sqrt(nodes)
    value = np.sin(2.0 * np.pi * root) / root
    return tuple(float(c) for c in np.polynomial.polynomial.polyfit(nodes, value, 5))


SINE = sine_coefficients()


def sine_of(u):
    square = u * u
    total = jnp.full_like(u, SINE[-1])
    for c in SINE[-2::-1]:
        total = total * square + c
    return total * u


def cos_sin_of(turns):
    rest = turns - jnp.round(turns)
    cos = sine_of(0.25 - jnp.abs(rest))
    sin = sine_of(jnp.maximum(jnp.minimum(rest, 0.5 - rest), -0.5 - rest))
    return cos, sin


def pack_kernel(positions_ref, columns_ref, out_ref):
    row_groups, far, tiles = out_ref.shape[0], out_ref.shape[1], positions_ref.shape[0]
    quarter, width = (out_ref.shape[2] - 1) // tiles, columns_ref.shape[0]
    mine = positions_ref[lax.axis_index(FAR)].astype(jnp.float32).astype(out_ref.dtype)
    nothing = jnp.zeros((2, LANES), out_ref.dtype)
    for r in range(row_groups):
        for c in range(quarter):
            column = r * quarter + c
            for t in range(tiles):
                part = columns_ref[column, :, t * LANES : (t + 1) * LANES] if column < width else nothing
                for d in range(far):
                    out_ref[r, d, t * quarter + c] = part
        for d in range(far):
            out_ref[r, d, tiles * quarter] = mine


def packed(positions, columns, row_groups, far):
    width, tiles = columns.shape[0], positions.shape[0]
    assert tiles == far
    pairs = tiles * -(-width // row_groups) + 1
    return pl.pallas_call(
        pack_kernel,
        out_shape=jax.ShapeDtypeStruct((row_groups, far, pairs, 2, LANES), columns.dtype),
        in_specs=[pl.BlockSpec(memory_space=pltpu.VMEM)] * 2,
        out_specs=pl.BlockSpec(memory_space=pltpu.VMEM),
        cost_estimate=pl.CostEstimate(flops=2**16, bytes_accessed=0, transcendentals=0),
        compiler_params=pltpu.CompilerParams(vmem_limit_bytes=2**20),
        name="pack",
    )(positions, columns)


def tables_kernel(*refs):
    *angles, table_ref, turns = refs
    side, share = len(angles), angles[0].shape[1]
    blocks = turns.shape[1]
    each = share // LANES
    for s, ref in enumerate(angles):
        first = lax.rem(lax.axis_index(SIDE) + side - s, side) * each
        part = ref[...].astype(jnp.float32) * (1.0 / PHASES)
        for j in range(each):
            for k in range(2):
                turns[k, pl.ds(first + j, 1), :] = part[k : k + 1, j * LANES : (j + 1) * LANES]

    def fill(step, carry):
        for k in range(2):
            cos, sin = cos_sin_of(turns[k] * step.astype(jnp.float32))
            first = pl.multiple_of(2 * step * blocks, 2 * blocks)
            table_ref[k, pl.ds(first, blocks), :] = cos
            table_ref[k, pl.ds(first + blocks, blocks), :] = sin
        return carry

    lax.fori_loop(0, LATTICE, fill, 0, unroll=4)


def tables_of(angles):
    blocks = len(angles) * angles[0].shape[1] // LANES
    return pl.pallas_call(
        tables_kernel,
        out_shape=jax.ShapeDtypeStruct((2, LATTICE * 2 * blocks, LANES), jnp.float32),
        in_specs=[pl.BlockSpec(memory_space=pltpu.VMEM)] * len(angles),
        out_specs=pl.BlockSpec(memory_space=pltpu.VMEM),
        scratch_shapes=[pltpu.VMEM((2, blocks, LANES), jnp.float32)],
        cost_estimate=pl.CostEstimate(flops=2**22, bytes_accessed=0, transcendentals=0),
        compiler_params=pltpu.CompilerParams(vmem_limit_bytes=4 * 2**20),
        name="tables",
    )(*angles)


def steering_kernel(own_ref, table_ref, out_ref, stage, listed, rows, arrived):
    row_groups, tiles, pairs, _, _ = own_ref.shape
    blocks, elements = out_ref.shape[1:3]
    for r in range(row_groups):
        for t in range(tiles):
            part = (own_ref[r, t, pairs - 1].astype(jnp.float32) * (2 * blocks)).astype(jnp.int32)
            for k in range(2):
                here = k * elements + (r * tiles + t) * LANES
                listed[here : here + LANES] = part[k]
    copy = pltpu.make_async_copy(listed, rows, arrived)
    copy.start()
    copy.wait()

    def batch(step, carry):
        first = pl.multiple_of(step * BATCH, BATCH)
        for e in range(BATCH):
            one = pl.multiple_of(rows[first + e], 2 * blocks)
            two = pl.multiple_of(rows[elements + first + e], 2 * blocks)
            cos_one, sin_one = jnp.split(table_ref[0, pl.ds(one, 2 * blocks), :], 2)
            cos_two, sin_two = jnp.split(table_ref[1, pl.ds(two, 2 * blocks), :], 2)
            here = pl.ds(e, blocks, stride=PITCH)
            stage[0, here, :] = cos_one * cos_two - sin_one * sin_two
            stage[1, here, :] = sin_one * cos_two + cos_one * sin_two
        for k in range(2):
            for b in range(blocks):
                part = stage[k, b * PITCH : b * PITCH + BATCH, :]
                out_ref[k, b, pl.ds(first, BATCH), :] = part.astype(out_ref.dtype)
        return carry

    lax.fori_loop(0, elements // BATCH, batch, 0)


def steering_of(own, table):
    blocks = table.shape[1] // (2 * LATTICE)
    elements = own.shape[0] * own.shape[1] * LANES
    return pl.pallas_call(
        steering_kernel,
        out_shape=pltpu.VMEM((2, blocks, elements, LANES), own.dtype),
        in_specs=[pl.BlockSpec(memory_space=pltpu.VMEM)] * 2,
        out_specs=pl.BlockSpec(memory_space=pltpu.VMEM),
        scratch_shapes=[
            pltpu.VMEM((2, blocks * PITCH, LANES), jnp.float32),
            pltpu.VMEM((2 * elements,), jnp.int32),
            pltpu.SMEM((2 * elements,), jnp.int32),
            pltpu.SemaphoreType.DMA,
        ],
        cost_estimate=pl.CostEstimate(
            flops=64 * blocks * elements * LANES, bytes_accessed=0, transcendentals=0
        ),
        compiler_params=pltpu.CompilerParams(vmem_limit_bytes=6 * 2**20),
        name="steering",
    )(own, table)


def sums_kernel(*refs):
    *pieces, steering_ref, out_ref = refs
    row_groups, far, pairs, _, _ = pieces[0].shape
    tiles = steering_ref.shape[2] // (row_groups * LANES)
    quarter = (pairs - 1) // tiles
    weights = [
        [
            ref[r, d, t * quarter : (t + 1) * quarter].reshape(2 * quarter, LANES)
            for r in range(row_groups)
            for t in range(tiles)
        ]
        for ref in pieces
        for d in range(far)
    ]
    weights = jnp.concatenate([jnp.concatenate(part, 1) for part in weights], 0)
    is_real = lax.broadcasted_iota(jnp.int32, (8, LANES), 0) % 2 == 0
    for b in range(out_ref.shape[0]):
        both = jnp.concatenate([steering_ref[0, b], steering_ref[1, b]], 1)
        product = jnp.dot(weights, both, preferred_element_type=jnp.float32)
        total = jnp.zeros((8, LANES), jnp.float32)
        for g in range(0, product.shape[0], 8):
            cos, sin = product[g : g + 8, :LANES], product[g : g + 8, LANES:]
            real = cos + pltpu.roll(sin, 7, 0)
            imag = sin - pltpu.roll(cos, 7, 0)
            total = total + (real * real + imag * imag)
        out_ref[b : b + 1, :] = jnp.sum(jnp.where(is_real, total, 0.0), 0, keepdims=True)


def sums_of(pieces, steering):
    blocks = steering.shape[1]
    return pl.pallas_call(
        sums_kernel,
        out_shape=jax.ShapeDtypeStruct((blocks, LANES), jnp.float32),
        in_specs=[pl.BlockSpec(memory_space=pltpu.VMEM)] * (len(pieces) + 1),
        out_specs=pl.BlockSpec(memory_space=pltpu.VMEM),
        cost_estimate=pl.CostEstimate(
            flops=8 * len(pieces) * pieces[0].size * blocks * LANES,
            bytes_accessed=0,
            transcendentals=0,
        ),
        compiler_params=pltpu.CompilerParams(vmem_limit_bytes=6 * 2**20),
        name="sums",
    )(*pieces, steering)


def spectrum_of(positions, angles, subspace):
    rows, side, far = lax.axis_size(ROWS), lax.axis_size(SIDE), lax.axis_size(FAR)
    tiles = positions.shape[1] // LANES
    coordinates = positions.reshape(2, tiles, LANES).transpose(1, 0, 2)
    pieces = packed(coordinates, subspace.transpose(2, 0, 1), rows, far)
    own = lax.all_to_all(
        pieces.reshape(rows * far, *pieces.shape[2:]), (ROWS, FAR), 0, 0, tiled=True
    )
    turned = [angles]
    for step in range(1, side):
        moves = [(s, (s + step) % side) for s in range(side)]
        turned.append(lax.ppermute(angles, SIDE, moves))
    shared = [
        lax.ppermute(own, NEAR, [(0, 1), (1, 0)]),
        lax.ppermute(own, (NEAR, CORE), [(0, 3), (3, 0), (1, 2), (2, 1)]),
        lax.ppermute(own, CORE, [(0, 1), (1, 0)]),
    ]
    own, *shared = (part.reshape(pieces.shape) for part in (own, *shared))

    steering = steering_of(own, tables_of(turned))
    sums = sums_of((own, *shared), steering).reshape(1, side, -1)
    sums = jnp.broadcast_to(sums, (rows, *sums.shape[1:]))
    parts = lax.all_to_all(sums.reshape(rows * side, -1), (ROWS, SIDE), 0, 0, tiled=True)
    return 1.0 / (jnp.sum(parts, 0) / NOISE + 1e-06)


def solution(mesh):
    split = Mesh(mesh.devices.reshape(mesh.shape["rows"], 4, 2, 4, 2), (ROWS, *GRID))
    in_specs = (P(None, ROWS), P(None, GRID), P(None, ROWS, GRID))
    return jax.shard_map(spectrum_of, mesh=split, in_specs=in_specs, out_specs=P(GRID), check_vma=False)
```

```python
import jax
import jax.numpy as jnp
import numpy as np
from jax import lax
from jax.experimental import pallas as pl
from jax.experimental.pallas import tpu as pltpu
from jax.sharding import Mesh
from jax.sharding import PartitionSpec as P

NOISE = 1920
PHASES = 4096
LATTICE = 64
LANES = 128
BATCH = 32
PITCH = BATCH + 4
ROWS, FAR, NEAR, SIDE, CORE = "rows", "far", "near", "side", "core"
GRID = (FAR, NEAR, SIDE, CORE)


def sine_coefficients():
    nodes = 0.03125 * (1.0 - np.cos((np.arange(64) + 0.5) * np.pi / 64))
    root = np.sqrt(nodes)
    value = np.sin(2.0 * np.pi * root) / root
    return tuple(float(c) for c in np.polynomial.polynomial.polyfit(nodes, value, 5))


SINE = sine_coefficients()


def sine_of(u):
    square = u * u
    total = jnp.full_like(u, SINE[-1])
    for c in SINE[-2::-1]:
        total = total * square + c
    return total * u


def cos_sin_of(turns):
    rest = turns - jnp.round(turns)
    cos = sine_of(0.25 - jnp.abs(rest))
    sin = sine_of(jnp.maximum(jnp.minimum(rest, 0.5 - rest), -0.5 - rest))
    return cos, sin


def pack_kernel(positions_hbm, angles_hbm, columns_hbm, out_ref, turns_ref, positions, angles, columns, sems):
    pairs = ((positions_hbm, positions), (angles_hbm, angles), (columns_hbm, columns))
    copies = [pltpu.make_async_copy(*pair, sems.at[k]) for k, pair in enumerate(pairs)]
    for copy in copies:
        copy.start()
    for copy in copies:
        copy.wait()
    row_groups, far, tiles = out_ref.shape[0], out_ref.shape[1], positions.shape[0]
    quarter, width = (out_ref.shape[2] - 1) // tiles, columns.shape[0]
    turns_ref[...] = angles[...].astype(jnp.float32) * (1.0 / PHASES)
    mine = positions[lax.axis_index(FAR)].astype(jnp.float32).astype(out_ref.dtype)
    nothing = jnp.zeros((2, LANES), out_ref.dtype)
    for r in range(row_groups):
        for c in range(quarter):
            column = r * quarter + c
            for t in range(tiles):
                part = columns[column, :, t * LANES : (t + 1) * LANES] if column < width else nothing
                for d in range(far):
                    out_ref[r, d, t * quarter + c] = part
        for d in range(far):
            out_ref[r, d, tiles * quarter] = mine


def packed(positions, angles, columns, row_groups, far):
    width, tiles = columns.shape[0], positions.shape[0]
    assert tiles == far
    pairs = tiles * -(-width // row_groups) + 1
    return pl.pallas_call(
        pack_kernel,
        out_shape=(
            jax.ShapeDtypeStruct((row_groups, far, pairs, 2, LANES), columns.dtype),
            jax.ShapeDtypeStruct(angles.shape, jnp.float32),
        ),
        in_specs=[pl.BlockSpec(memory_space=pltpu.HBM)] * 3,
        out_specs=[pl.BlockSpec(memory_space=pltpu.VMEM)] * 2,
        scratch_shapes=[
            pltpu.VMEM(positions.shape, positions.dtype),
            pltpu.VMEM(angles.shape, angles.dtype),
            pltpu.VMEM(columns.shape, columns.dtype),
            pltpu.SemaphoreType.DMA((3,)),
        ],
        cost_estimate=pl.CostEstimate(flops=2**16, bytes_accessed=0, transcendentals=0),
        compiler_params=pltpu.CompilerParams(vmem_limit_bytes=2 * 2**20),
        name="pack",
    )(*(pltpu.with_memory_space_constraint(part, pltpu.HBM) for part in (positions, angles, columns)))


def tables_kernel(*refs):
    *parts, table_ref, turns = refs
    side, share = len(parts), parts[0].shape[1]
    blocks = turns.shape[1]
    each = share // LANES
    for s, ref in enumerate(parts):
        first = lax.rem(lax.axis_index(SIDE) + side - s, side) * each
        part = ref[...]
        for j in range(each):
            for k in range(2):
                turns[k, pl.ds(first + j, 1), :] = part[k : k + 1, j * LANES : (j + 1) * LANES]

    def fill(step, carry):
        for k in range(2):
            cos, sin = cos_sin_of(turns[k] * step.astype(jnp.float32))
            first = pl.multiple_of(2 * step * blocks, 2 * blocks)
            table_ref[k, pl.ds(first, blocks), :] = cos
            table_ref[k, pl.ds(first + blocks, blocks), :] = sin
        return carry

    lax.fori_loop(0, LATTICE, fill, 0, unroll=4)


def tables_of(parts):
    blocks = len(parts) * parts[0].shape[1] // LANES
    return pl.pallas_call(
        tables_kernel,
        out_shape=jax.ShapeDtypeStruct((2, LATTICE * 2 * blocks, LANES), jnp.float32),
        in_specs=[pl.BlockSpec(memory_space=pltpu.VMEM)] * len(parts),
        out_specs=pl.BlockSpec(memory_space=pltpu.VMEM),
        scratch_shapes=[pltpu.VMEM((2, blocks, LANES), jnp.float32)],
        cost_estimate=pl.CostEstimate(flops=2**22, bytes_accessed=0, transcendentals=0),
        compiler_params=pltpu.CompilerParams(vmem_limit_bytes=4 * 2**20),
        name="tables",
    )(*parts)


def steering_kernel(own_ref, table_ref, out_ref, stage, listed, rows, arrived):
    row_groups, tiles, pairs, _, _ = own_ref.shape
    blocks, elements = out_ref.shape[1:3]
    for r in range(row_groups):
        for t in range(tiles):
            part = (own_ref[r, t, pairs - 1].astype(jnp.float32) * (2 * blocks)).astype(jnp.int32)
            for k in range(2):
                here = k * elements + (r * tiles + t) * LANES
                listed[here : here + LANES] = part[k]
    copy = pltpu.make_async_copy(listed, rows, arrived)
    copy.start()
    copy.wait()

    def batch(step, carry):
        first = pl.multiple_of(step * BATCH, BATCH)
        for e in range(BATCH):
            one = pl.multiple_of(rows[first + e], 2 * blocks)
            two = pl.multiple_of(rows[elements + first + e], 2 * blocks)
            cos_one, sin_one = jnp.split(table_ref[0, pl.ds(one, 2 * blocks), :], 2)
            cos_two, sin_two = jnp.split(table_ref[1, pl.ds(two, 2 * blocks), :], 2)
            here = pl.ds(e, blocks, stride=PITCH)
            stage[0, here, :] = cos_one * cos_two - sin_one * sin_two
            stage[1, here, :] = sin_one * cos_two + cos_one * sin_two
        for k in range(2):
            for b in range(blocks):
                part = stage[k, b * PITCH : b * PITCH + BATCH, :]
                out_ref[k, b, pl.ds(first, BATCH), :] = part.astype(out_ref.dtype)
        return carry

    lax.fori_loop(0, elements // BATCH, batch, 0)


def steering_of(own, table):
    blocks = table.shape[1] // (2 * LATTICE)
    elements = own.shape[0] * own.shape[1] * LANES
    return pl.pallas_call(
        steering_kernel,
        out_shape=pltpu.VMEM((2, blocks, elements, LANES), own.dtype),
        in_specs=[pl.BlockSpec(memory_space=pltpu.VMEM)] * 2,
        out_specs=pl.BlockSpec(memory_space=pltpu.VMEM),
        scratch_shapes=[
            pltpu.VMEM((2, blocks * PITCH, LANES), jnp.float32),
            pltpu.VMEM((2 * elements,), jnp.int32),
            pltpu.SMEM((2 * elements,), jnp.int32),
            pltpu.SemaphoreType.DMA,
        ],
        cost_estimate=pl.CostEstimate(
            flops=64 * blocks * elements * LANES, bytes_accessed=0, transcendentals=0
        ),
        compiler_params=pltpu.CompilerParams(vmem_limit_bytes=6 * 2**20),
        name="steering",
    )(own, table)


def sums_kernel(*refs):
    *pieces, steering_ref, out_ref = refs
    row_groups, far, pairs, _, _ = pieces[0].shape
    tiles = steering_ref.shape[2] // (row_groups * LANES)
    quarter = (pairs - 1) // tiles
    weights = [
        [
            ref[r, d, t * quarter : (t + 1) * quarter].reshape(2 * quarter, LANES)
            for r in range(row_groups)
            for t in range(tiles)
        ]
        for ref in pieces
        for d in range(far)
    ]
    weights = jnp.concatenate([jnp.concatenate(part, 1) for part in weights], 0)
    is_real = lax.broadcasted_iota(jnp.int32, (8, LANES), 0) % 2 == 0
    for b in range(out_ref.shape[0]):
        both = jnp.concatenate([steering_ref[0, b], steering_ref[1, b]], 1)
        product = jnp.dot(weights, both, preferred_element_type=jnp.float32)
        total = jnp.zeros((8, LANES), jnp.float32)
        for g in range(0, product.shape[0], 8):
            cos, sin = product[g : g + 8, :LANES], product[g : g + 8, LANES:]
            real = cos + pltpu.roll(sin, 7, 0)
            imag = sin - pltpu.roll(cos, 7, 0)
            total = total + (real * real + imag * imag)
        out_ref[b : b + 1, :] = jnp.sum(jnp.where(is_real, total, 0.0), 0, keepdims=True)


def sums_of(pieces, steering):
    blocks = steering.shape[1]
    return pl.pallas_call(
        sums_kernel,
        out_shape=jax.ShapeDtypeStruct((blocks, LANES), jnp.float32),
        in_specs=[pl.BlockSpec(memory_space=pltpu.VMEM)] * (len(pieces) + 1),
        out_specs=pl.BlockSpec(memory_space=pltpu.VMEM),
        cost_estimate=pl.CostEstimate(
            flops=8 * len(pieces) * pieces[0].size * blocks * LANES,
            bytes_accessed=0,
            transcendentals=0,
        ),
        compiler_params=pltpu.CompilerParams(vmem_limit_bytes=6 * 2**20),
        name="sums",
    )(*pieces, steering)


def spectrum_of(positions, angles, subspace):
    rows, side, far = lax.axis_size(ROWS), lax.axis_size(SIDE), lax.axis_size(FAR)
    tiles = positions.shape[1] // LANES
    coordinates = positions.reshape(2, tiles, LANES).transpose(1, 0, 2)
    pieces, turns = packed(coordinates, angles, subspace.transpose(2, 0, 1), rows, far)
    own = lax.all_to_all(
        pieces.reshape(rows * far, *pieces.shape[2:]), (ROWS, FAR), 0, 0, tiled=True
    )
    turned = [turns]
    for step in range(1, side):
        moves = [(s, (s + step) % side) for s in range(side)]
        turned.append(lax.ppermute(turns, SIDE, moves))
    cores = [(0, 1), (1, 0)]
    along = lax.ppermute(own, NEAR, [(0, 1), (1, 0)])
    across = lax.ppermute(own, CORE, cores)
    both = lax.ppermute(along, CORE, cores)
    own, *shared = (part.reshape(pieces.shape) for part in (own, along, across, both))

    steering = steering_of(own, tables_of(turned))
    sums = sums_of((own, *shared), steering).reshape(1, side, -1)
    sums = jnp.broadcast_to(sums, (rows, *sums.shape[1:]))
    parts = lax.all_to_all(sums.reshape(rows * side, -1), (ROWS, SIDE), 0, 0, tiled=True)
    return 1.0 / (jnp.sum(parts, 0) / NOISE + 1e-06)


def solution(mesh):
    split = Mesh(mesh.devices.reshape(mesh.shape["rows"], 4, 2, 4, 2), (ROWS, *GRID))
    in_specs = (P(None, ROWS), P(None, GRID), P(None, ROWS, GRID))
    return jax.shard_map(spectrum_of, mesh=split, in_specs=in_specs, out_specs=P(GRID), check_vma=False)
```

```python
import jax
import jax.numpy as jnp
import numpy as np
from jax import lax
from jax.experimental import pallas as pl
from jax.experimental.pallas import tpu as pltpu
from jax.sharding import Mesh
from jax.sharding import PartitionSpec as P

NOISE = 1920
PHASES = 4096
LATTICE = 64
LANES = 128
BATCH = 128
PITCH = BATCH + 4
ROWS, FAR, NEAR, SIDE, CORE = "rows", "far", "near", "side", "core"
GRID = (FAR, NEAR, SIDE, CORE)


def sine_coefficients():
    nodes = 0.03125 * (1.0 - np.cos((np.arange(64) + 0.5) * np.pi / 64))
    root = np.sqrt(nodes)
    value = np.sin(2.0 * np.pi * root) / root
    return tuple(float(c) for c in np.polynomial.polynomial.polyfit(nodes, value, 5))


SINE = sine_coefficients()


def sine_of(u):
    square = u * u
    total = jnp.full_like(u, SINE[-1])
    for c in SINE[-2::-1]:
        total = total * square + c
    return total * u


def cos_sin_of(turns):
    rest = turns - jnp.round(turns)
    cos = sine_of(0.25 - jnp.abs(rest))
    sin = sine_of(jnp.maximum(jnp.minimum(rest, 0.5 - rest), -0.5 - rest))
    return cos, sin


def pack_kernel(positions_hbm, angles_hbm, columns_hbm, out_ref, turns_ref, positions, angles, columns, sems):
    pairs = ((positions_hbm, positions), (angles_hbm, angles), (columns_hbm, columns))
    copies = [pltpu.make_async_copy(*pair, sems.at[k]) for k, pair in enumerate(pairs)]
    for copy in copies:
        copy.start()
    for copy in copies:
        copy.wait()
    row_groups, far, tiles = out_ref.shape[0], out_ref.shape[1], positions.shape[0]
    quarter, width = (out_ref.shape[2] - 1) // tiles, columns.shape[0]
    turns_ref[...] = angles[...].astype(jnp.float32) * (1.0 / PHASES)
    mine = positions[lax.axis_index(FAR)].astype(jnp.float32).astype(out_ref.dtype)
    nothing = jnp.zeros((2, LANES), out_ref.dtype)
    for r in range(row_groups):
        for c in range(quarter):
            column = r * quarter + c
            for t in range(tiles):
                part = columns[column, :, t * LANES : (t + 1) * LANES] if column < width else nothing
                for d in range(far):
                    out_ref[r, d, t * quarter + c] = part
        for d in range(far):
            out_ref[r, d, tiles * quarter] = mine


def packed(positions, angles, columns, row_groups, far):
    width, tiles = columns.shape[0], positions.shape[0]
    assert tiles == far
    pairs = tiles * -(-width // row_groups) + 1
    return pl.pallas_call(
        pack_kernel,
        out_shape=(
            jax.ShapeDtypeStruct((row_groups, far, pairs, 2, LANES), columns.dtype),
            jax.ShapeDtypeStruct(angles.shape, jnp.float32),
        ),
        in_specs=[pl.BlockSpec(memory_space=pltpu.HBM)] * 3,
        out_specs=[pl.BlockSpec(memory_space=pltpu.VMEM)] * 2,
        scratch_shapes=[
            pltpu.VMEM(positions.shape, positions.dtype),
            pltpu.VMEM(angles.shape, angles.dtype),
            pltpu.VMEM(columns.shape, columns.dtype),
            pltpu.SemaphoreType.DMA((3,)),
        ],
        cost_estimate=pl.CostEstimate(flops=2**16, bytes_accessed=0, transcendentals=0),
        compiler_params=pltpu.CompilerParams(vmem_limit_bytes=2 * 2**20),
        name="pack",
    )(*(pltpu.with_memory_space_constraint(part, pltpu.HBM) for part in (positions, angles, columns)))


def tables_kernel(*refs):
    *parts, table_ref, turns = refs
    share, blocks = parts[0].shape[1], turns.shape[1]
    each = share // LANES
    for s, ref in enumerate(parts):
        first = (lax.axis_index(SIDE) ^ s) * each
        part = ref[...]
        for j in range(each):
            for k in range(2):
                turns[k, pl.ds(first + j, 1), :] = part[k : k + 1, j * LANES : (j + 1) * LANES]

    def fill(step, carry):
        for k in range(2):
            cos, sin = cos_sin_of(turns[k] * step.astype(jnp.float32))
            first = pl.multiple_of(2 * step * blocks, 2 * blocks)
            table_ref[k, pl.ds(first, blocks), :] = cos
            table_ref[k, pl.ds(first + blocks, blocks), :] = sin
        return carry

    lax.fori_loop(0, LATTICE, fill, 0, unroll=4)


def tables_of(parts):
    blocks = len(parts) * parts[0].shape[1] // LANES
    return pl.pallas_call(
        tables_kernel,
        out_shape=jax.ShapeDtypeStruct((2, LATTICE * 2 * blocks, LANES), jnp.float32),
        in_specs=[pl.BlockSpec(memory_space=pltpu.VMEM)] * len(parts),
        out_specs=pl.BlockSpec(memory_space=pltpu.VMEM),
        scratch_shapes=[pltpu.VMEM((2, blocks, LANES), jnp.float32)],
        cost_estimate=pl.CostEstimate(flops=2**22, bytes_accessed=0, transcendentals=0),
        compiler_params=pltpu.CompilerParams(vmem_limit_bytes=4 * 2**20),
        name="tables",
    )(*parts)


def steering_kernel(own_ref, table_ref, out_ref, stage, listed, rows, arrived):
    row_groups, tiles, pairs, _, _ = own_ref.shape
    blocks, elements = out_ref.shape[1:3]
    for r in range(row_groups):
        for t in range(tiles):
            part = (own_ref[r, t, pairs - 1].astype(jnp.float32) * (2 * blocks)).astype(jnp.int32)
            for k in range(2):
                here = k * elements + (r * tiles + t) * LANES
                listed[here : here + LANES] = part[k]
    copy = pltpu.make_async_copy(listed, rows, arrived)
    copy.start()
    copy.wait()

    def batch(step, carry):
        first = pl.multiple_of(step * BATCH, BATCH)
        for e in range(BATCH):
            one = pl.multiple_of(rows[first + e], 2 * blocks)
            two = pl.multiple_of(rows[elements + first + e], 2 * blocks)
            cos_one, sin_one = jnp.split(table_ref[0, pl.ds(one, 2 * blocks), :], 2)
            cos_two, sin_two = jnp.split(table_ref[1, pl.ds(two, 2 * blocks), :], 2)
            here = pl.ds(e, blocks, stride=PITCH)
            stage[0, here, :] = cos_one * cos_two - sin_one * sin_two
            stage[1, here, :] = sin_one * cos_two + cos_one * sin_two
        for k in range(2):
            for b in range(blocks):
                part = stage[k, b * PITCH : b * PITCH + BATCH, :]
                out_ref[k, b, pl.ds(first, BATCH), :] = part.astype(out_ref.dtype)
        return carry

    lax.fori_loop(0, elements // BATCH, batch, 0)


def steering_of(own, table):
    blocks = table.shape[1] // (2 * LATTICE)
    elements = own.shape[0] * own.shape[1] * LANES
    return pl.pallas_call(
        steering_kernel,
        out_shape=pltpu.VMEM((2, blocks, elements, LANES), own.dtype),
        in_specs=[pl.BlockSpec(memory_space=pltpu.VMEM)] * 2,
        out_specs=pl.BlockSpec(memory_space=pltpu.VMEM),
        scratch_shapes=[
            pltpu.VMEM((2, blocks * PITCH, LANES), jnp.float32),
            pltpu.VMEM((2 * elements,), jnp.int32),
            pltpu.SMEM((2 * elements,), jnp.int32),
            pltpu.SemaphoreType.DMA,
        ],
        cost_estimate=pl.CostEstimate(
            flops=64 * blocks * elements * LANES, bytes_accessed=0, transcendentals=0
        ),
        compiler_params=pltpu.CompilerParams(vmem_limit_bytes=6 * 2**20),
        name="steering",
    )(own, table)


def sums_kernel(*refs):
    *pieces, steering_ref, out_ref = refs
    row_groups, far, pairs, _, _ = pieces[0].shape
    tiles = steering_ref.shape[2] // (row_groups * LANES)
    quarter = (pairs - 1) // tiles
    weights = [
        [
            ref[r, d, t * quarter : (t + 1) * quarter].reshape(2 * quarter, LANES)
            for r in range(row_groups)
            for t in range(tiles)
        ]
        for ref in pieces
        for d in range(far)
    ]
    weights = jnp.concatenate([jnp.concatenate(part, 1) for part in weights], 0)
    is_real = lax.broadcasted_iota(jnp.int32, (8, LANES), 0) % 2 == 0
    for b in range(out_ref.shape[0]):
        both = jnp.concatenate([steering_ref[0, b], steering_ref[1, b]], 1)
        product = jnp.dot(weights, both, preferred_element_type=jnp.float32)
        total = jnp.zeros((8, LANES), jnp.float32)
        for g in range(0, product.shape[0], 8):
            cos, sin = product[g : g + 8, :LANES], product[g : g + 8, LANES:]
            real = cos + pltpu.roll(sin, 7, 0)
            imag = sin - pltpu.roll(cos, 7, 0)
            total = total + (real * real + imag * imag)
        out_ref[b : b + 1, :] = jnp.sum(jnp.where(is_real, total, 0.0), 0, keepdims=True)


def sums_of(pieces, steering):
    blocks = steering.shape[1]
    return pl.pallas_call(
        sums_kernel,
        out_shape=jax.ShapeDtypeStruct((blocks, LANES), jnp.float32),
        in_specs=[pl.BlockSpec(memory_space=pltpu.VMEM)] * (len(pieces) + 1),
        out_specs=pl.BlockSpec(memory_space=pltpu.VMEM),
        cost_estimate=pl.CostEstimate(
            flops=8 * len(pieces) * pieces[0].size * blocks * LANES,
            bytes_accessed=0,
            transcendentals=0,
        ),
        compiler_params=pltpu.CompilerParams(vmem_limit_bytes=6 * 2**20),
        name="sums",
    )(*pieces, steering)


def spectrum_of(positions, angles, subspace):
    rows, side, far = lax.axis_size(ROWS), lax.axis_size(SIDE), lax.axis_size(FAR)
    tiles = positions.shape[1] // LANES
    coordinates = positions.reshape(2, tiles, LANES).transpose(1, 0, 2)
    pieces, turns = packed(coordinates, angles, subspace.transpose(2, 0, 1), rows, far)
    own = lax.all_to_all(
        pieces.reshape(rows * far, *pieces.shape[2:]), (ROWS, FAR), 0, 0, tiled=True
    )
    turned = [turns]
    for step in range(1, side):
        moves = [(s, s ^ step) for s in range(side)]
        turned.append(lax.ppermute(turns, SIDE, moves))
    cores = [(0, 1), (1, 0)]
    along = lax.ppermute(own, NEAR, [(0, 1), (1, 0)])
    across = lax.ppermute(own, CORE, cores)
    both = lax.ppermute(along, CORE, cores)
    own, *shared = (part.reshape(pieces.shape) for part in (own, along, across, both))

    steering = steering_of(own, tables_of(turned))
    sums = sums_of((own, *shared), steering).reshape(1, side, -1)
    sums = jnp.broadcast_to(sums, (rows, *sums.shape[1:]))
    parts = lax.all_to_all(sums.reshape(rows * side, -1), (ROWS, SIDE), 0, 0, tiled=True)
    return 1.0 / (jnp.sum(parts, 0) / NOISE + 1e-06)


def solution(mesh):
    split = Mesh(mesh.devices.reshape(mesh.shape["rows"], 4, 2, 4, 2), (ROWS, *GRID))
    in_specs = (P(None, ROWS), P(None, GRID), P(None, ROWS, GRID))
    return jax.shard_map(spectrum_of, mesh=split, in_specs=in_specs, out_specs=P(GRID), check_vma=False)
```

```python
import jax
import jax.numpy as jnp
import numpy as np
from jax import lax
from jax.experimental import pallas as pl
from jax.experimental.pallas import tpu as pltpu
from jax.sharding import Mesh
from jax.sharding import PartitionSpec as P

NOISE = 1920
PHASES = 4096
LATTICE = 64
LANES = 128
BATCH = 256
PITCH = BATCH + 4
ROWS, FAR, NEAR, SIDE, CORE = "rows", "far", "near", "side", "core"
GRID = (FAR, NEAR, SIDE, CORE)


def sine_coefficients():
    nodes = 0.03125 * (1.0 - np.cos((np.arange(64) + 0.5) * np.pi / 64))
    root = np.sqrt(nodes)
    value = np.sin(2.0 * np.pi * root) / root
    return tuple(float(c) for c in np.polynomial.polynomial.polyfit(nodes, value, 5))


SINE = sine_coefficients()


def sine_of(u):
    square = u * u
    total = jnp.full_like(u, SINE[-1])
    for c in SINE[-2::-1]:
        total = total * square + c
    return total * u


def cos_sin_of(turns):
    rest = turns - jnp.round(turns)
    cos = sine_of(0.25 - jnp.abs(rest))
    sin = sine_of(jnp.maximum(jnp.minimum(rest, 0.5 - rest), -0.5 - rest))
    return cos, sin


def pack_kernel(positions_hbm, angles_hbm, columns_hbm, out_ref, turns_ref, positions, angles, columns, sems):
    pairs = ((positions_hbm, positions), (angles_hbm, angles), (columns_hbm, columns))
    copies = [pltpu.make_async_copy(*pair, sems.at[k]) for k, pair in enumerate(pairs)]
    for copy in copies:
        copy.start()
    for copy in copies:
        copy.wait()
    row_groups, far, tiles = out_ref.shape[0], out_ref.shape[1], positions.shape[0]
    quarter, width = (out_ref.shape[2] - 1) // tiles, columns.shape[0]
    turns_ref[...] = angles[...].astype(jnp.float32) * (1.0 / PHASES)
    mine = positions[lax.axis_index(FAR)].astype(jnp.float32).astype(out_ref.dtype)
    nothing = jnp.zeros((2, LANES), out_ref.dtype)
    for r in range(row_groups):
        for c in range(quarter):
            column = r * quarter + c
            for t in range(tiles):
                part = columns[column, :, t * LANES : (t + 1) * LANES] if column < width else nothing
                for d in range(far):
                    out_ref[r, d, t * quarter + c] = part
        for d in range(far):
            out_ref[r, d, tiles * quarter] = mine


def packed(positions, angles, columns, row_groups, far):
    width, tiles = columns.shape[0], positions.shape[0]
    assert tiles == far
    pairs = tiles * -(-width // row_groups) + 1
    return pl.pallas_call(
        pack_kernel,
        out_shape=(
            jax.ShapeDtypeStruct((row_groups, far, pairs, 2, LANES), columns.dtype),
            jax.ShapeDtypeStruct(angles.shape, jnp.float32),
        ),
        in_specs=[pl.BlockSpec(memory_space=pltpu.HBM)] * 3,
        out_specs=[pl.BlockSpec(memory_space=pltpu.VMEM)] * 2,
        scratch_shapes=[
            pltpu.VMEM(positions.shape, positions.dtype),
            pltpu.VMEM(angles.shape, angles.dtype),
            pltpu.VMEM(columns.shape, columns.dtype),
            pltpu.SemaphoreType.DMA((3,)),
        ],
        cost_estimate=pl.CostEstimate(flops=2**16, bytes_accessed=0, transcendentals=0),
        compiler_params=pltpu.CompilerParams(vmem_limit_bytes=2 * 2**20),
        name="pack",
    )(*(pltpu.with_memory_space_constraint(part, pltpu.HBM) for part in (positions, angles, columns)))


def tables_kernel(*refs):
    *parts, table_ref, turns = refs
    share, blocks = parts[0].shape[1], turns.shape[1]
    each = share // LANES
    for s, ref in enumerate(parts):
        first = (lax.axis_index(SIDE) ^ s) * each
        part = ref[...]
        for j in range(each):
            for k in range(2):
                turns[k, pl.ds(first + j, 1), :] = part[k : k + 1, j * LANES : (j + 1) * LANES]

    def fill(step, carry):
        for k in range(2):
            cos, sin = cos_sin_of(turns[k] * step.astype(jnp.float32))
            first = pl.multiple_of(2 * step * blocks, 2 * blocks)
            table_ref[k, pl.ds(first, blocks), :] = cos
            table_ref[k, pl.ds(first + blocks, blocks), :] = sin
        return carry

    lax.fori_loop(0, LATTICE, fill, 0, unroll=4)


def tables_of(parts):
    blocks = len(parts) * parts[0].shape[1] // LANES
    return pl.pallas_call(
        tables_kernel,
        out_shape=jax.ShapeDtypeStruct((2, LATTICE * 2 * blocks, LANES), jnp.float32),
        in_specs=[pl.BlockSpec(memory_space=pltpu.VMEM)] * len(parts),
        out_specs=pl.BlockSpec(memory_space=pltpu.VMEM),
        scratch_shapes=[pltpu.VMEM((2, blocks, LANES), jnp.float32)],
        cost_estimate=pl.CostEstimate(flops=2**22, bytes_accessed=0, transcendentals=0),
        compiler_params=pltpu.CompilerParams(vmem_limit_bytes=4 * 2**20),
        name="tables",
    )(*parts)


def steering_kernel(own_ref, table_ref, out_ref, stage, listed, rows, arrived):
    row_groups, tiles, pairs, _, _ = own_ref.shape
    blocks, elements = out_ref.shape[1:3]
    for r in range(row_groups):
        for t in range(tiles):
            part = (own_ref[r, t, pairs - 1].astype(jnp.float32) * (2 * blocks)).astype(jnp.int32)
            for k in range(2):
                here = k * elements + (r * tiles + t) * LANES
                listed[here : here + LANES] = part[k]
    early = BATCH * 2
    spans = [(0, early), (elements, early), (early, elements - early), (elements + early, elements - early)]
    copies = [
        pltpu.make_async_copy(listed.at[pl.ds(*span)], rows.at[pl.ds(*span)], arrived.at[k])
        for k, span in enumerate(spans)
    ]
    for copy in copies:
        copy.start()
    for copy in copies[:2]:
        copy.wait()

    def batch(step, carry):
        first = pl.multiple_of(step * BATCH, BATCH)
        for e in range(BATCH):
            one = pl.multiple_of(rows[first + e], 2 * blocks)
            two = pl.multiple_of(rows[elements + first + e], 2 * blocks)
            cos_one, sin_one = jnp.split(table_ref[0, pl.ds(one, 2 * blocks), :], 2)
            cos_two, sin_two = jnp.split(table_ref[1, pl.ds(two, 2 * blocks), :], 2)
            here = pl.ds(e, blocks, stride=PITCH)
            stage[0, here, :] = cos_one * cos_two - sin_one * sin_two
            stage[1, here, :] = sin_one * cos_two + cos_one * sin_two
        for k in range(2):
            for b in range(blocks):
                part = stage[k, b * PITCH : b * PITCH + BATCH, :]
                out_ref[k, b, pl.ds(first, BATCH), :] = part.astype(out_ref.dtype)
        return carry

    lax.fori_loop(0, early // BATCH, batch, 0)
    for copy in copies[2:]:
        copy.wait()
    lax.fori_loop(early // BATCH, elements // BATCH, batch, 0)


def steering_of(own, table):
    blocks = table.shape[1] // (2 * LATTICE)
    elements = own.shape[0] * own.shape[1] * LANES
    return pl.pallas_call(
        steering_kernel,
        out_shape=pltpu.VMEM((2, blocks, elements, LANES), own.dtype),
        in_specs=[pl.BlockSpec(memory_space=pltpu.VMEM)] * 2,
        out_specs=pl.BlockSpec(memory_space=pltpu.VMEM),
        scratch_shapes=[
            pltpu.VMEM((2, blocks * PITCH, LANES), jnp.float32),
            pltpu.VMEM((2 * elements,), jnp.int32),
            pltpu.SMEM((2 * elements,), jnp.int32),
            pltpu.SemaphoreType.DMA((4,)),
        ],
        cost_estimate=pl.CostEstimate(
            flops=64 * blocks * elements * LANES, bytes_accessed=0, transcendentals=0
        ),
        compiler_params=pltpu.CompilerParams(vmem_limit_bytes=6 * 2**20),
        name="steering",
    )(own, table)


def sums_kernel(*refs):
    *pieces, steering_ref, out_ref = refs
    row_groups, far, pairs, _, _ = pieces[0].shape
    tiles = steering_ref.shape[2] // (row_groups * LANES)
    quarter = (pairs - 1) // tiles
    weights = [
        [
            ref[r, d, t * quarter : (t + 1) * quarter].reshape(2 * quarter, LANES)
            for r in range(row_groups)
            for t in range(tiles)
        ]
        for ref in pieces
        for d in range(far)
    ]
    weights = jnp.concatenate([jnp.concatenate(part, 1) for part in weights], 0)
    is_real = lax.broadcasted_iota(jnp.int32, (8, LANES), 0) % 2 == 0
    for b in range(out_ref.shape[0]):
        both = jnp.concatenate([steering_ref[0, b], steering_ref[1, b]], 1)
        product = jnp.dot(weights, both, preferred_element_type=jnp.float32)
        total = jnp.zeros((8, LANES), jnp.float32)
        for g in range(0, product.shape[0], 8):
            cos, sin = product[g : g + 8, :LANES], product[g : g + 8, LANES:]
            real = cos + pltpu.roll(sin, 7, 0)
            imag = sin - pltpu.roll(cos, 7, 0)
            total = total + (real * real + imag * imag)
        out_ref[b : b + 1, :] = jnp.sum(jnp.where(is_real, total, 0.0), 0, keepdims=True)


def sums_of(pieces, steering):
    blocks = steering.shape[1]
    return pl.pallas_call(
        sums_kernel,
        out_shape=jax.ShapeDtypeStruct((blocks, LANES), jnp.float32),
        in_specs=[pl.BlockSpec(memory_space=pltpu.VMEM)] * (len(pieces) + 1),
        out_specs=pl.BlockSpec(memory_space=pltpu.VMEM),
        cost_estimate=pl.CostEstimate(
            flops=8 * len(pieces) * pieces[0].size * blocks * LANES,
            bytes_accessed=0,
            transcendentals=0,
        ),
        compiler_params=pltpu.CompilerParams(vmem_limit_bytes=6 * 2**20),
        name="sums",
    )(*pieces, steering)


def spectrum_of(positions, angles, subspace):
    rows, side, far = lax.axis_size(ROWS), lax.axis_size(SIDE), lax.axis_size(FAR)
    tiles = positions.shape[1] // LANES
    coordinates = positions.reshape(2, tiles, LANES).transpose(1, 0, 2)
    pieces, turns = packed(coordinates, angles, subspace.transpose(2, 0, 1), rows, far)
    own = lax.all_to_all(
        pieces.reshape(rows * far, *pieces.shape[2:]), (ROWS, FAR), 0, 0, tiled=True
    )
    turned = [turns]
    for step in range(1, side):
        moves = [(s, s ^ step) for s in range(side)]
        turned.append(lax.ppermute(turns, SIDE, moves))
    cores = [(0, 1), (1, 0)]
    along = lax.ppermute(own, NEAR, [(0, 1), (1, 0)])
    across = lax.ppermute(own, CORE, cores)
    both = lax.ppermute(along, CORE, cores)
    own, *shared = (part.reshape(pieces.shape) for part in (own, along, across, both))

    steering = steering_of(own, tables_of(turned))
    sums = sums_of((own, *shared), steering).reshape(1, side, -1)
    sums = jnp.broadcast_to(sums, (rows, *sums.shape[1:]))
    parts = lax.all_to_all(sums.reshape(rows * side, -1), (ROWS, SIDE), 0, 0, tiled=True)
    return 1.0 / (jnp.sum(parts, 0) / NOISE + 1e-06)


def solution(mesh):
    split = Mesh(mesh.devices.reshape(mesh.shape["rows"], 4, 2, 4, 2), (ROWS, *GRID))
    in_specs = (P(None, ROWS), P(None, GRID), P(None, ROWS, GRID))
    return jax.shard_map(spectrum_of, mesh=split, in_specs=in_specs, out_specs=P(GRID), check_vma=False)
```
